32 devices in a mesh: groups: 1, row: 32 (over z, y, x, core).
Axes of the slice: x: 2, y: 2, z: 4, core: 2. Of those that a mesh axis runs over, the one named last changes fastest.
Arguments:
- sub_vectors: float32 [8192, 2, 8192], P('groups', None, 'row'), may hold values from -6 to 6
- eigen_values: float32 [2, 8192], P(None, ('groups', 'row')), may hold values from -16384 to 16384, as said below
- kept: int32 [2, 8192], P(None, ('groups', 'row')), may hold values from 0 to 1, as said below
- poles: int32 [2, 128], P(None, 'groups'), may hold values from 0 to 16383, as said below
- coupling: float32 [1], P('groups'), may hold values from 0.5 to 2
Outputs:
- position: float32 [128], P('groups')
- merged: float32 [8192, 2, 128], P(('groups', 'row'))
The draws below stay inside these ranges and needn't reach their ends.
Inputs may be any that keep to these rules, and one draw needn't show every extreme that they name: `kept`: exactly 4096 entries are 0. All named entries are kept; poles[0, k] and poles[1, k] are neighbours among the kept eigenvalues in increasing order, poles[1, k] the larger; with S = 96, the rank of poles[0, k] among the kept eigenvalues (rank 0 the smallest) lies between k * S and (k + 1) * S - 2. `eigen_values`: all distinct; neighbouring values in sorted order differ by 0.25 or more.
All inputs are finite; a program needn't handle non-finite values.
Results may differ from the reference program's by a relative error of at most 0.0003.
Values sent between devices are 32-bit elements; how exact they have to be, the bound alone decides.
A program may use at most 128 MiB of HBM per device.

```python
import math
import jax
import jax.numpy as jnp
from jax import lax

HALF = 8192
ORDER = 16384
ROOTS = 128
ITERS = 5


def structure(key):
    order = jax.random.permutation(jax.random.fold_in(key, 11), ORDER).astype(jnp.int32)
    dropped = jax.random.permutation(jax.random.fold_in(key, 12), ORDER)[:ORDER // 4]
    kept_sorted = jnp.ones((ORDER,), jnp.int32).at[dropped].set(0)
    kept_count = ORDER - ORDER // 4
    stride = kept_count // ROOTS
    sort_keys = jnp.where(kept_sorted == 1, 0, ORDER) + jnp.arange(ORDER, dtype=jnp.int32)
    kept_places = jnp.argsort(sort_keys)[:kept_count].astype(jnp.int32)
    jitter = jax.random.randint(jax.random.fold_in(key, 13), (ROOTS,), 0, stride - 1)
    ranks = (jnp.arange(ROOTS, dtype=jnp.int32) * stride + jitter).astype(jnp.int32)
    lower_place = kept_places[ranks]
    upper_place = kept_places[ranks + 1]
    kept_all = jnp.zeros((ORDER,), jnp.int32).at[order].set(kept_sorted)
    pole_index = jnp.stack([order[lower_place], order[upper_place]]).astype(jnp.int32)
    return (order, kept_all, pole_index)


def draw_eigen_values(key, part):
    order, kept_all, pole_index = structure(key)
    gap_key = jax.random.fold_in(key, 14)
    gaps = jax.random.uniform(gap_key, (ORDER,), jnp.float32, 0.5, 1.5)
    values = jnp.cumsum(gaps)
    values = values - 0.5 * values[-1]
    spread = jnp.zeros((ORDER,), jnp.float32).at[order].set(values)
    return spread.reshape(2, HALF)


def draw_kept(key, part):
    order, kept_all, pole_index = structure(key)
    return kept_all.reshape(2, HALF)


def draw_poles(key, part):
    order, kept_all, pole_index = structure(key)
    return pole_index


def block_levels(rng, dims, cuts, low, top_value):
    gain = 1.0
    for dim, shards_of in cuts:
        heights = jax.random.uniform(jax.random.fold_in(jax.random.fold_in(rng, 6), dim), (shards_of,), jnp.float32, low / len(cuts), top_value / len(cuts))
        gain = gain * jnp.repeat(jnp.exp(heights), dims[dim] // shards_of).reshape((-1,) + (1,) * (len(dims) - 1 - dim))
    return gain


def noise(rng, shape, width, limit, split=(), kind=jnp.bfloat16):
    array = jax.random.normal(rng, shape, jnp.float32) * width
    if len(split) > 0:
        array = block_levels(rng, shape, split, -0.22, 0.18) * array
    return jnp.clip(array, min=-limit, max=limit).astype(kind)


def setup_inputs(seed: int = 0, part: int = 0) -> dict:
    keys = jax.random.split(jax.random.key(seed), 6)
    part_splits = jax.random.split(jax.random.fold_in(keys[5], part), 6)
    sub_vectors = noise(part_splits[0], (HALF, 2, HALF), 1.0, 6.0, ((2, 32),), jnp.float32)
    eigen_values = draw_eigen_values(jax.random.fold_in(jax.random.fold_in(keys[5], part), 71), part)
    kept = draw_kept(jax.random.fold_in(jax.random.fold_in(keys[5], part), 71), part)
    poles = draw_poles(jax.random.fold_in(jax.random.fold_in(keys[5], part), 71), part)
    coupling = jnp.clip(jnp.exp(jax.random.uniform(part_splits[4], (1,), jnp.float32, math.log(0.5), math.log(2.0))), 0.5, 2.0)
    return {"sub_vectors": sub_vectors, "eigen_values": eigen_values, "kept": kept, "poles": poles, "coupling": coupling}


def secular_terms(weights, shifted, offset):
    inverse = 1.0 / (shifted - offset[:, None])
    part = weights[None, :] * inverse
    return (lax.optimization_barrier(jnp.sum(part, 1)), lax.optimization_barrier(jnp.sum(part * inverse, 1)))

def reference(sub_vectors, eigen_values, kept, poles, coupling):
    kept_float = kept.astype(jnp.float32)
    boundary = jnp.stack([sub_vectors[HALF - 1, 0, :], sub_vectors[0, 1, :]])
    masked_z = boundary * kept_float
    masked_d = eigen_values - 1000000.0 * (1.0 - kept_float)
    flat_d = masked_d.reshape(-1)
    pole_values = flat_d[poles]
    lower = pole_values[0]
    spacing = pole_values[1] - lower
    weights = (masked_z * masked_z).reshape(-1)
    shifted = flat_d[None, :] - lower[:, None]
    offset = 0.5 * spacing
    for step in range(ITERS):
        total, slope = secular_terms(weights, shifted, offset)
        moved = offset - (1.0 / coupling[0] + total) / slope
        offset = jnp.clip(moved, 0.02 * spacing, 0.98 * spacing)
    unused, norm_sq = secular_terms(weights, shifted, offset)
    position = offset / spacing
    normalizer = 1.0 / jnp.sqrt(norm_sq)
    vectors = masked_z[:, :, None] / (masked_d[:, :, None] - lower - offset) * normalizer
    merged = jnp.einsum('isj,sjk->isk', sub_vectors, vectors, precision=lax.Precision.HIGHEST)
    return (position, merged)
```

```python
import functools

import jax
import jax.numpy as jnp
from jax import lax
from jax.experimental import pallas as pl
from jax.experimental.pallas import tpu as pltpu
from jax.sharding import PartitionSpec as P

ITERS = 5
MESH = pl.DeviceIdType.MESH
LANES = 128


def total_of(x):
    return jnp.sum(jnp.sum(x, axis=0, keepdims=True), axis=1, keepdims=True)


def kernel(
    n,
    inner_chips,
    packed,
    portion,
    poles,
    coupling,
    payload,
    index,
    z_column,
    d_column,
    sub,
    position,
    merged,
    gathered,
    full_z,
    full_d,
    own_roots,
    roots,
    held,
    factors,
    partial,
    partner_partial,
    mine,
    arrived,
    reduced_a,
    reduced_b,
    last_a,
    last_b,
    load_sem,
    gather_send,
    gather_recv,
    roots_send,
    roots_recv,
    pair_send,
    pair_recv,
    first_send,
    first_recv,
    a_send,
    a_recv,
    b_send,
    b_recv,
):
    me = lax.axis_index("row")
    chips = n // 2
    core = lax.rem(me, 2)
    chip = me // 2
    size_a = inner_chips
    size_b = chips // size_a
    place_a = lax.rem(chip, size_a)
    place_b = chip // size_a
    rows, root_total = partial.shape[2], partial.shape[3]
    tile_rows = sub.shape[0] // (rows * n)
    blocks = tile_rows // 2
    columns = blocks * LANES
    loads = load_sem.shape[0]
    load_rows = sub.shape[0] // loads

    def load(i):
        part = pl.ds(pl.multiple_of(i * load_rows, 8), load_rows)
        return pltpu.make_async_copy(sub.at[part], held.at[part], load_sem.at[i])

    for i in range(loads):
        load(i).start()

    barrier = pltpu.get_barrier_semaphore()

    def greet(i, carry):
        pl.semaphore_signal(barrier, inc=1, device_id={"row": lax.rem(me + i, n)}, device_id_type=MESH)
        return carry

    lax.fori_loop(1, n, greet, 0)
    pl.semaphore_wait(barrier, n - 1)

    def push(source, target, send, recv):
        def step(i, carry):
            pltpu.make_async_remote_copy(
                src_ref=source,
                dst_ref=target.at[i - 1],
                send_sem=send,
                recv_sem=recv,
                device_id={"row": lax.rem(me + i, n)},
                device_id_type=MESH,
            ).start()
            return carry

        lax.fori_loop(1, n, step, 0)

    def settle(target, sem):
        whole = target.at[pl.ds(0, n - 1)]
        pltpu.make_async_copy(whole, whole, sem).wait()

    push(payload, gathered, gather_send, gather_recv)
    settle(gathered, gather_recv)
    half = payload.shape[0] // 2
    full_z[pl.ds(0, packed), :] = payload[pl.ds(0, packed), :]
    full_d[pl.ds(0, packed), :] = payload[pl.ds(half, packed), :]
    for i in range(1, n):
        full_z[pl.ds(i * packed, packed), :] = gathered[i - 1, pl.ds(0, packed), :]
        full_d[pl.ds(i * packed, packed), :] = gathered[i - 1, pl.ds(half, packed), :]
    values = full_d[...]
    weights = full_z[...] * full_z[...]
    slot = index[0]
    within = index[1]
    owner = lax.rem(me - slot + n, n)
    places = within + owner * columns
    inverse_coupling = 1.0 / coupling[0]
    lane = lax.broadcasted_iota(jnp.int32, (1, root_total), 1)
    rows_out = [jnp.zeros((1, root_total), jnp.float32) for _ in range(4)]
    for r in range(portion):
        k = me * portion + r
        lower = total_of(jnp.where(places == poles[0, k], values, 0.0))
        spacing = total_of(jnp.where(places == poles[1, k], values, 0.0)) - lower
        shifted = values - lower
        offset = 0.5 * spacing
        for step in range(ITERS + 1):
            inverse = 1.0 / (shifted - offset)
            part = weights * inverse
            slope = total_of(part * inverse)
            if step < ITERS:
                moved = offset - (inverse_coupling + total_of(part)) / slope
                offset = jnp.minimum(jnp.maximum(moved, 0.02 * spacing), 0.98 * spacing)
        for i, value in enumerate((lower, spacing, offset, slope)):
            rows_out[i] = jnp.where(lane == k, value, rows_out[i])
    for i in range(4):
        own_roots[pl.ds(i, 1), :] = rows_out[i]
    own_roots[pl.ds(4, 4), :] = jnp.zeros((4, root_total), jnp.float32)
    push(own_roots, roots, roots_send, roots_recv)
    settle(roots, roots_recv)
    known = own_roots[...]
    for i in range(n - 1):
        known = known + roots[i]
    lower, spacing, offset, norm_sq = (known[i : i + 1, :] for i in range(4))
    position[...] = offset / spacing
    vectors = z_column[...] / ((d_column[...] - lower) - offset) * (1.0 / jnp.sqrt(norm_sq))
    top = vectors.astype(jnp.bfloat16)
    factors[:, pl.ds(0, root_total)] = top
    factors[:, pl.ds(root_total, root_total)] = (vectors - top.astype(jnp.float32)).astype(jnp.bfloat16)

    for i in range(loads):
        load(i).wait()

    outer = (size_b, size_a)
    inner = (size_a, size_b)

    def target_chip(s, u, v):
        step_a, step_b = (v, u) if s == 0 else (u, v)
        new_a = lax.rem(place_a + step_a + 1, size_a)
        new_b = lax.rem(place_b + step_b + 1, size_b)
        return new_a, new_b

    def product(s, device):
        start = device * (rows * tile_rows)
        pieces = [held[pl.ds(start + j * 2 + s, rows, stride=tile_rows), :] for j in range(blocks)]
        a = pieces[0] if blocks == 1 else jnp.concatenate(pieces, axis=1)
        high = a.astype(jnp.bfloat16)
        low = (a - high.astype(jnp.float32)).astype(jnp.bfloat16)
        right = factors[pl.ds(s * columns, columns), :]
        both = jnp.dot(high, right, preferred_element_type=jnp.float32)
        small = jnp.dot(low, right[:, :root_total], preferred_element_type=jnp.float32)
        return both[:, :root_total] + (both[:, root_total:] + small)

    def pair_copy(s, t):
        return pltpu.make_async_remote_copy(
            src_ref=partial.at[s, t],
            dst_ref=partner_partial.at[s, t],
            send_sem=pair_send.at[s, t],
            recv_sem=pair_recv.at[s, t],
            device_id={"row": chip * 2 + 1 - core},
            device_id_type=MESH,
        )

    def first_copy(s, t):
        u, v = t // inner[s], lax.rem(t, inner[s])
        new_a, new_b = target_chip(s, u, v)
        peer = place_b * size_a + new_a if s == 0 else new_b * size_a + place_a
        return pltpu.make_async_remote_copy(
            src_ref=mine.at[s, t],
            dst_ref=arrived.at[s, t],
            send_sem=first_send.at[s, t],
            recv_sem=first_recv.at[s, t],
            device_id={"row": peer * 2 + core},
            device_id_type=MESH,
        )

    def device_of(s, t, which):
        new_a, new_b = target_chip(s, t // inner[s], lax.rem(t, inner[s]))
        return (new_b * size_a + new_a) * 2 + which

    def for_partner(t, carry):
        for s in range(2):
            partial[s, t] = product(s, device_of(s, t, 1 - core))
            pair_copy(s, t).start()
        return carry

    lax.fori_loop(0, chips, for_partner, 0)

    def for_self(t, carry):
        for s in range(2):
            value = product(s, device_of(s, t, core))
            pair_copy(s, t).wait_recv()
            mine[s, t] = value + partner_partial[s, t]

            @pl.when(lax.rem(t, inner[s]) != inner[s] - 1)
            def _():
                first_copy(s, t).start()

        return carry

    lax.fori_loop(0, chips, for_self, 0)

    reduced, last = (reduced_a, reduced_b), (last_a, last_b)
    sends, recvs = (a_send, b_send), (a_recv, b_recv)

    def second_copy(s, u):
        new_a, new_b = target_chip(s, u, u)
        peer = new_b * size_a + place_a if s == 0 else place_b * size_a + new_a
        return pltpu.make_async_remote_copy(
            src_ref=reduced[s].at[u],
            dst_ref=last[s].at[u],
            send_sem=sends[s].at[u],
            recv_sem=recvs[s].at[u],
            device_id={"row": peer * 2 + core},
            device_id_type=MESH,
        )

    def fold(s, u):
        base = u * inner[s]
        value = mine[s, base + inner[s] - 1]
        for v in range(inner[s] - 1):
            first_copy(s, base + v).wait_recv()
            value = value + arrived[s, base + v]
        reduced[s][u] = value

    for u in range(max(outer)):
        for s in range(2):
            if u < outer[s]:
                fold(s, u)
                if u < outer[s] - 1:
                    second_copy(s, u).start()

    for s in range(2):
        value = reduced[s][outer[s] - 1]
        for u in range(outer[s] - 1):
            second_copy(s, u).wait_recv()
            value = value + last[s][u]
        strips = root_total // LANES
        for strip in range(strips):
            merged[pl.ds(strip * 2 + s, rows, stride=2 * strips), :] = value[:, strip * LANES : (strip + 1) * LANES]

    settle(gathered, gather_send)
    settle(roots, roots_send)

    def drain(t, carry):
        for s in range(2):
            pair_copy(s, t).wait_send()

            @pl.when(lax.rem(t, inner[s]) != inner[s] - 1)
            def _():
                first_copy(s, t).wait_send()

        return carry

    lax.fori_loop(0, chips, drain, 0)
    for s in range(2):
        for u in range(outer[s] - 1):
            second_copy(s, u).wait_send()


def body(sub_vectors, eigen_values, kept, poles, coupling):
    order, _, columns = sub_vectors.shape
    n = lax.axis_size("row")
    root_total = poles.shape[1]
    portion = root_total // n
    strips = root_total // LANES
    rows = order // n
    chips = n // 2
    inner_chips = 4 if chips % 4 == 0 else 1
    outer_chips = chips // inner_chips
    blocks = columns // LANES
    packed = 2 * blocks
    half = -(-packed // 4) * 4

    kept_float = kept.astype(jnp.float32)
    boundary = jnp.stack([sub_vectors[order - 1, 0, :], sub_vectors[0, 1, :]])
    masked_z = boundary * kept_float
    masked_d = eigen_values - 1000000.0 * (1.0 - kept_float)
    tall = lambda x: jnp.pad(x.reshape(packed, LANES), ((0, half - packed), (0, 0)))
    payload = jnp.concatenate([tall(masked_z), tall(masked_d)], axis=0)
    slot = jnp.broadcast_to(jnp.arange(n, dtype=jnp.int32)[:, None, None], (n, packed, LANES))
    within = (
        jnp.arange(2, dtype=jnp.int32)[:, None] * order + jnp.arange(columns, dtype=jnp.int32)[None, :]
    ).reshape(1, packed, LANES)
    within = jnp.broadcast_to(within, (n, packed, LANES))
    index = jnp.stack([slot, within]).reshape(2, n * packed, LANES)
    view = (
        sub_vectors.reshape(order, 2, blocks, LANES)
        .transpose(0, 2, 1, 3)
        .reshape(order * blocks * 2, LANES)
    )
    vmem = pl.BlockSpec(memory_space=pltpu.VMEM)
    smem = pl.BlockSpec(memory_space=pltpu.SMEM)
    chunk = (rows, root_total)
    f32 = jnp.float32
    dma = pltpu.SemaphoreType.DMA
    position, merged = pl.pallas_call(
        functools.partial(kernel, n, inner_chips, packed, portion),
        out_shape=(
            jax.ShapeDtypeStruct((1, root_total), f32),
            jax.ShapeDtypeStruct((rows * 2 * strips, LANES), f32),
        ),
        in_specs=[smem, smem, vmem, vmem, vmem, vmem, pl.BlockSpec(memory_space=pl.ANY)],
        out_specs=(vmem, vmem),
        scratch_shapes=[
            pltpu.VMEM((n - 1, 2 * half, LANES), f32),
            pltpu.VMEM((n * packed, LANES), f32),
            pltpu.VMEM((n * packed, LANES), f32),
            pltpu.VMEM((8, root_total), f32),
            pltpu.VMEM((n - 1, 8, root_total), f32),
            pltpu.VMEM(view.shape, f32),
            pltpu.VMEM((2 * columns, 2 * root_total), jnp.bfloat16),
            pltpu.VMEM((2, chips) + chunk, f32),
            pltpu.VMEM((2, chips) + chunk, f32),
            pltpu.VMEM((2, chips) + chunk, f32),
            pltpu.VMEM((2, chips) + chunk, f32),
            pltpu.VMEM((outer_chips,) + chunk, f32),
            pltpu.VMEM((inner_chips,) + chunk, f32),
            pltpu.VMEM((outer_chips,) + chunk, f32),
            pltpu.VMEM((inner_chips,) + chunk, f32),
            dma((8,)),
            dma,
            dma,
            dma,
            dma,
            dma((2, chips)),
            dma((2, chips)),
            dma((2, chips)),
            dma((2, chips)),
            dma((outer_chips,)),
            dma((outer_chips,)),
            dma((inner_chips,)),
            dma((inner_chips,)),
        ],
        compiler_params=pltpu.CompilerParams(
            collective_id=0, has_side_effects=True, vmem_limit_bytes=60 * 1024 * 1024
        ),
    )(
        poles,
        coupling,
        payload,
        index,
        masked_z.reshape(-1, 1),
        masked_d.reshape(-1, 1),
        view,
    )
    merged = merged.reshape(rows, strips, 2, LANES).transpose(0, 2, 1, 3).reshape(rows, 2, root_total)
    return (position.reshape(root_total), merged)


def solution(mesh):
    in_specs = (
        P("groups", None, "row"),
        P(None, ("groups", "row")),
        P(None, ("groups", "row")),
        P(None, "groups"),
        P("groups"),
    )
    out_specs = (P("groups"), P(("groups", "row"), None, None))
    return jax.shard_map(body, mesh=mesh, in_specs=in_specs, out_specs=out_specs, check_vma=False)
```

```python
import functools

import jax
import jax.numpy as jnp
from jax import lax
from jax.experimental import pallas as pl
from jax.experimental.pallas import tpu as pltpu
from jax.sharding import PartitionSpec as P

ITERS = 5
MESH = pl.DeviceIdType.MESH
LANES = 128


def total_of(x):
    return jnp.sum(jnp.sum(x, axis=0, keepdims=True), axis=1, keepdims=True)


def kernel(
    n,
    inner_chips,
    packed,
    portion,
    poles,
    coupling,
    payload,
    sub,
    position,
    merged,
    gathered,
    full_z,
    full_d,
    own_roots,
    roots,
    held,
    factors,
    partial,
    partner_partial,
    mine,
    arrived,
    reduced_a,
    reduced_b,
    last_a,
    last_b,
    load_sem,
    gather_send,
    gather_recv,
    roots_send,
    roots_recv,
    pair_send,
    pair_recv,
    first_send,
    first_recv,
    second_send,
    second_recv,
):
    me = lax.axis_index("row")
    chips = n // 2
    core = lax.rem(me, 2)
    chip = me // 2
    size_a = inner_chips
    size_b = chips // size_a
    place_a = lax.rem(chip, size_a)
    place_b = chip // size_a
    rows, root_total = partial.shape[2], partial.shape[3]
    tile_rows = sub.shape[0] // (rows * n)
    blocks = tile_rows // 2
    columns = blocks * LANES
    loads = load_sem.shape[0]
    load_rows = sub.shape[0] // loads

    def load(i):
        part = pl.ds(pl.multiple_of(i * load_rows, 8), load_rows)
        return pltpu.make_async_copy(sub.at[part], held.at[part], load_sem.at[i])

    for i in range(loads):
        load(i).start()

    barrier = pltpu.get_barrier_semaphore()

    def greet(i, carry):
        pl.semaphore_signal(barrier, inc=1, device_id={"row": lax.rem(me + i, n)}, device_id_type=MESH)
        return carry

    lax.fori_loop(1, n, greet, 0)
    pl.semaphore_wait(barrier, n - 1)

    def push(source, target, send, recv):
        def step(i, carry):
            pltpu.make_async_remote_copy(
                src_ref=source,
                dst_ref=target.at[i - 1],
                send_sem=send,
                recv_sem=recv,
                device_id={"row": lax.rem(me + i, n)},
                device_id_type=MESH,
            ).start()
            return carry

        lax.fori_loop(1, n, step, 0)

    def settle(target, sem):
        whole = target.at[pl.ds(0, n - 1)]
        pltpu.make_async_copy(whole, whole, sem).wait()

    push(payload, gathered, gather_send, gather_recv)
    padding = jnp.zeros((LANES - payload.shape[0], LANES), jnp.float32)
    standing = jnp.transpose(jnp.concatenate([payload[...], padding], axis=0))
    settle(gathered, gather_recv)
    half = payload.shape[0] // 2
    full_z[pl.ds(0, packed), :] = payload[pl.ds(0, packed), :]
    full_d[pl.ds(0, packed), :] = payload[pl.ds(half, packed), :]
    for i in range(1, n):
        full_z[pl.ds(i * packed, packed), :] = gathered[i - 1, pl.ds(0, packed), :]
        full_d[pl.ds(i * packed, packed), :] = gathered[i - 1, pl.ds(half, packed), :]
    values = full_d[...]
    weights = full_z[...] * full_z[...]
    line = lax.broadcasted_iota(jnp.int32, (n * packed, LANES), 0)
    slot = lax.shift_right_logical(line, jnp.full_like(line, packed.bit_length() - 1))
    line = line - slot * packed
    side = jnp.where(line >= blocks, 1, 0)
    owner = me - slot
    owner = jnp.where(owner < 0, owner + n, owner)
    order = rows * n
    places = side * order + owner * columns + (line - side * blocks) * LANES
    places = places + lax.broadcasted_iota(jnp.int32, (n * packed, LANES), 1)
    inverse_coupling = 1.0 / coupling[0]
    lane = lax.broadcasted_iota(jnp.int32, (1, root_total), 1)
    rows_out = [jnp.zeros((1, root_total), jnp.float32) for _ in range(4)]
    for r in range(portion):
        k = me * portion + r
        lower = total_of(jnp.where(places == poles[0, k], values, 0.0))
        spacing = total_of(jnp.where(places == poles[1, k], values, 0.0)) - lower
        shifted = values - lower
        offset = 0.5 * spacing
        for step in range(ITERS + 1):
            inverse = 1.0 / (shifted - offset)
            part = weights * inverse
            slope = total_of(part * inverse)
            if step < ITERS:
                moved = offset - (inverse_coupling + total_of(part)) / slope
                offset = jnp.minimum(jnp.maximum(moved, 0.02 * spacing), 0.98 * spacing)
        for i, value in enumerate((lower, spacing, offset, slope)):
            rows_out[i] = jnp.where(lane == k, value, rows_out[i])
    for i in range(4):
        own_roots[pl.ds(i, 1), :] = rows_out[i]
    own_roots[pl.ds(4, 4), :] = jnp.zeros((4, root_total), jnp.float32)
    push(own_roots, roots, roots_send, roots_recv)
    settle(roots, roots_recv)
    known = own_roots[...]
    for i in range(n - 1):
        known = known + roots[i]
    lower, spacing, offset, norm_sq = (known[i : i + 1, :] for i in range(4))
    position[...] = offset / spacing
    normalizer = 1.0 / jnp.sqrt(norm_sq)
    for i in range(packed):
        piece = pl.ds(i * LANES, LANES)
        z_column = standing[:, i : i + 1]
        d_column = standing[:, half + i : half + i + 1]
        vectors = z_column / ((d_column - lower) - offset) * normalizer
        top = vectors.astype(jnp.bfloat16)
        factors[piece, pl.ds(0, root_total)] = top
        factors[piece, pl.ds(root_total, root_total)] = (vectors - top.astype(jnp.float32)).astype(jnp.bfloat16)

    for i in range(loads):
        load(i).wait()

    crossing = rows * 7 // 16 // 8 * 8
    parts = ((0, 0, rows, 0), (1, 0, rows - crossing, 0), (1, rows - crossing, crossing, 1))
    outer = (size_b, size_a)
    inner = (size_a, size_b)

    def target_chip(kind, u, v):
        step_a, step_b = (v, u) if kind == 0 else (u, v)
        new_a = lax.rem(place_a + step_a + 1, size_a)
        new_b = lax.rem(place_b + step_b + 1, size_b)
        return new_a, new_b

    def product(p, t, which):
        s, first, count, kind = parts[p]
        new_a, new_b = target_chip(kind, t // inner[kind], lax.rem(t, inner[kind]))
        device = (new_b * size_a + new_a) * 2 + which
        start = device * (rows * tile_rows) + first * tile_rows
        pieces = [held[pl.ds(start + j * 2 + s, count, stride=tile_rows), :] for j in range(blocks)]
        a = pieces[0] if blocks == 1 else jnp.concatenate(pieces, axis=1)
        high = a.astype(jnp.bfloat16)
        low = (a - high.astype(jnp.float32)).astype(jnp.bfloat16)
        right = factors[pl.ds(s * columns, columns), :]
        both = jnp.dot(high, right, preferred_element_type=jnp.float32)
        small = jnp.dot(low, right[:, :root_total], preferred_element_type=jnp.float32)
        return both[:, :root_total] + (both[:, root_total:] + small)

    def block(ref, p, t):
        s, first, count, kind = parts[p]
        return ref.at[s, t, pl.ds(first, count)]

    def pair_copy(p, t):
        return pltpu.make_async_remote_copy(
            src_ref=block(partial, p, t),
            dst_ref=block(partner_partial, p, t),
            send_sem=pair_send.at[p, t],
            recv_sem=pair_recv.at[p, t],
            device_id={"row": chip * 2 + 1 - core},
            device_id_type=MESH,
        )

    def first_copy(p, t):
        kind = parts[p][3]
        new_a, new_b = target_chip(kind, t // inner[kind], lax.rem(t, inner[kind]))
        peer = place_b * size_a + new_a if kind == 0 else new_b * size_a + place_a
        return pltpu.make_async_remote_copy(
            src_ref=block(mine, p, t),
            dst_ref=block(arrived, p, t),
            send_sem=first_send.at[p, t],
            recv_sem=first_recv.at[p, t],
            device_id={"row": peer * 2 + core},
            device_id_type=MESH,
        )

    def leaves(p, t):
        kind = parts[p][3]
        return lax.rem(t, inner[kind]) != inner[kind] - 1

    count_parts = len(parts)

    def for_partner(t):
        for p in range(count_parts):
            block(partial, p, t)[...] = product(p, t, 1 - core)
            pair_copy(p, t).start()

    def for_self(t):
        for p in range(count_parts):
            value = product(p, t, core)
            pair_copy(p, t).wait_recv()
            block(mine, p, t)[...] = value + block(partner_partial, p, t)[...]

            @pl.when(leaves(p, t))
            def _():
                first_copy(p, t).start()

    lead = min(2, chips)
    for t in range(lead):
        for_partner(t)

    def both_ways(t, carry):
        for_self(t)
        for_partner(t + lead)
        return carry

    lax.fori_loop(0, chips - lead, both_ways, 0)

    def rest(t, carry):
        for_self(t)
        return carry

    lax.fori_loop(chips - lead, chips, rest, 0)

    def second_block(refs, p, u):
        s, first, count, kind = parts[p]
        return refs[kind].at[s, u, pl.ds(first, count)] if kind == 0 else refs[kind].at[u]

    reduced, last = (reduced_a, reduced_b), (last_a, last_b)

    def second_copy(p, u):
        kind = parts[p][3]
        new_a, new_b = target_chip(kind, u, u)
        peer = new_b * size_a + place_a if kind == 0 else place_b * size_a + new_a
        return pltpu.make_async_remote_copy(
            src_ref=second_block(reduced, p, u),
            dst_ref=second_block(last, p, u),
            send_sem=second_send.at[p, u],
            recv_sem=second_recv.at[p, u],
            device_id={"row": peer * 2 + core},
            device_id_type=MESH,
        )

    def fold(p, u):
        kind = parts[p][3]
        base = u * inner[kind]
        value = block(mine, p, base + inner[kind] - 1)[...]
        for v in range(inner[kind] - 1):
            first_copy(p, base + v).wait_recv()
            value = value + block(arrived, p, base + v)[...]
        second_block(reduced, p, u)[...] = value

    for u in range(max(outer)):
        for p in range(count_parts):
            size = outer[parts[p][3]]
            if u < size:
                fold(p, u)
                if u < size - 1:
                    second_copy(p, u).start()

    strips = root_total // LANES
    for p in range(count_parts):
        s, first, count, kind = parts[p]
        value = second_block(reduced, p, outer[kind] - 1)[...]
        for u in range(outer[kind] - 1):
            second_copy(p, u).wait_recv()
            value = value + second_block(last, p, u)[...]
        for strip in range(strips):
            target = pl.ds((first * strips + strip) * 2 + s, count, stride=2 * strips)
            merged[target, :] = value[:, strip * LANES : (strip + 1) * LANES]

    settle(gathered, gather_send)
    settle(roots, roots_send)

    def drain(t, carry):
        for p in range(count_parts):
            pair_copy(p, t).wait_send()

            @pl.when(leaves(p, t))
            def _():
                first_copy(p, t).wait_send()

        return carry

    lax.fori_loop(0, chips, drain, 0)
    for p in range(count_parts):
        for u in range(outer[parts[p][3]] - 1):
            second_copy(p, u).wait_send()


def body(sub_vectors, eigen_values, kept, poles, coupling):
    order, _, columns = sub_vectors.shape
    n = lax.axis_size("row")
    root_total = poles.shape[1]
    portion = root_total // n
    strips = root_total // LANES
    rows = order // n
    chips = n // 2
    inner_chips = 4 if chips % 4 == 0 else 1
    outer_chips = chips // inner_chips
    blocks = columns // LANES
    packed = 2 * blocks
    half = -(-packed // 4) * 4

    kept_float = kept.astype(jnp.float32)
    boundary = jnp.stack([sub_vectors[order - 1, 0, :], sub_vectors[0, 1, :]])
    masked_z = boundary * kept_float
    masked_d = eigen_values - 1000000.0 * (1.0 - kept_float)
    tall = lambda x: jnp.pad(x.reshape(packed, LANES), ((0, half - packed), (0, 0)))
    payload = jnp.concatenate([tall(masked_z), tall(masked_d)], axis=0)
    view = (
        sub_vectors.reshape(order, 2, blocks, LANES)
        .transpose(0, 2, 1, 3)
        .reshape(order * blocks * 2, LANES)
    )
    vmem = pl.BlockSpec(memory_space=pltpu.VMEM)
    smem = pl.BlockSpec(memory_space=pltpu.SMEM)
    chunk = (rows, root_total)
    crossing = rows * 7 // 16 // 8 * 8
    f32 = jnp.float32
    dma = pltpu.SemaphoreType.DMA
    position, merged = pl.pallas_call(
        functools.partial(kernel, n, inner_chips, packed, portion),
        out_shape=(
            jax.ShapeDtypeStruct((1, root_total), f32),
            jax.ShapeDtypeStruct((rows * 2 * strips, LANES), f32),
        ),
        in_specs=[smem, smem, vmem, pl.BlockSpec(memory_space=pl.ANY)],
        out_specs=(vmem, vmem),
        scratch_shapes=[
            pltpu.VMEM((n - 1, 2 * half, LANES), f32),
            pltpu.VMEM((n * packed, LANES), f32),
            pltpu.VMEM((n * packed, LANES), f32),
            pltpu.VMEM((8, root_total), f32),
            pltpu.VMEM((n - 1, 8, root_total), f32),
            pltpu.VMEM(view.shape, f32),
            pltpu.VMEM((2 * columns, 2 * root_total), jnp.bfloat16),
            pltpu.VMEM((2, chips) + chunk, f32),
            pltpu.VMEM((2, chips) + chunk, f32),
            pltpu.VMEM((2, chips) + chunk, f32),
            pltpu.VMEM((2, chips) + chunk, f32),
            pltpu.VMEM((2, outer_chips) + chunk, f32),
            pltpu.VMEM((inner_chips, crossing, root_total), f32),
            pltpu.VMEM((2, outer_chips) + chunk, f32),
            pltpu.VMEM((inner_chips, crossing, root_total), f32),
            dma((8,)),
            dma,
            dma,
            dma,
            dma,
            dma((3, chips)),
            dma((3, chips)),
            dma((3, chips)),
            dma((3, chips)),
            dma((3, max(inner_chips, outer_chips))),
            dma((3, max(inner_chips, outer_chips))),
        ],
        compiler_params=pltpu.CompilerParams(
            collective_id=0, has_side_effects=True, vmem_limit_bytes=60 * 1024 * 1024
        ),
    )(
        poles,
        coupling,
        payload,
        view,
    )
    merged = merged.reshape(rows, strips, 2, LANES).transpose(0, 2, 1, 3).reshape(rows, 2, root_total)
    return (position.reshape(root_total), merged)


def solution(mesh):
    in_specs = (
        P("groups", None, "row"),
        P(None, ("groups", "row")),
        P(None, ("groups", "row")),
        P(None, "groups"),
        P("groups"),
    )
    out_specs = (P("groups"), P(("groups", "row"), None, None))
    return jax.shard_map(body, mesh=mesh, in_specs=in_specs, out_specs=out_specs, check_vma=False)
```
